32 devices in a mesh: ulysses: 8 (over z, x), blk: 4 (over y, core).
Axes of the slice: x: 2, y: 2, z: 4, core: 2. Of those that a mesh axis runs over, the one named last changes fastest.
Arguments:
- queries: bfloat16 [4, 512, 4096], P('blk', 'ulysses'), may hold values from -6 to 6
- key_rows: bfloat16 [4, 512, 1024], P('blk', 'ulysses'), may hold values from -6 to 6
- value_rows: bfloat16 [4, 512, 1024], P('blk', 'ulysses'), may hold values from -6 to 6
- tile_segment: int32 [16], replicated, may hold values from 0 to 3, never falling along the last dimension, each value on 1 to 8 neighbouring positions
Outputs:
- attended: bfloat16 [4, 512, 4096], P('blk', 'ulysses')
The draws below stay inside these ranges and needn't reach their ends.
Inputs may be any that keep to these rules, and one draw needn't show every extreme that they name: `tile_segment`: segment numbers never fall along the sequence and each segment covers 1 to 8 tiles.
All inputs are finite; a program needn't handle non-finite values.
Results may differ from the reference program's by a relative error of at most 0.0045.
Values may be sent and summed in bfloat16 or wider, within the bound.
A program may use at most 64 MiB of HBM per device.

```python
import math
import jax
import jax.numpy as jnp
import numpy as np
from jax import lax

Q_HEADS = 32
KV_HEADS = 8
HEAD_DIM = 128
TILE = 128
BLOCK_LEN = 512
BLOCKS = 4
TILES = 16


def draw_queries(key, part):
    seq_total = BLOCKS * BLOCK_LEN
    row_width = Q_HEADS * HEAD_DIM
    noise_key = jax.random.fold_in(key, 101)
    sample = jnp.clip(1.6 * jax.random.normal(noise_key, (seq_total, row_width), jnp.float32), -6.0, 6.0)
    return sample.reshape(BLOCKS, BLOCK_LEN, row_width).astype(jnp.bfloat16)


def draw_key_rows(key, part):
    seq_total = BLOCKS * BLOCK_LEN
    row_width = KV_HEADS * HEAD_DIM
    noise_key = jax.random.fold_in(key, 202)
    sample = jnp.clip(1.6 * jax.random.normal(noise_key, (seq_total, row_width), jnp.float32), -6.0, 6.0)
    return sample.reshape(BLOCKS, BLOCK_LEN, row_width).astype(jnp.bfloat16)


def block_levels(stream_key, extent, pieces, low, high):
    loudness = 1.0
    for axis_at, shards_of in pieces:
        draws = jax.random.uniform(jax.random.fold_in(jax.random.fold_in(stream_key, 6), axis_at), (shards_of,), jnp.float32, low / len(pieces), high / len(pieces))
        loudness = loudness * jnp.repeat(jnp.exp(draws), extent[axis_at] // shards_of).reshape((-1,) + (1,) * (len(extent) - 1 - axis_at))
    return loudness


def profile(amount, total, bound, skew):
    loads = [(1 << 20) // math.isqrt(standing ** skew) + 1 for standing in range(2, amount + 1)]
    rest, given = total - bound - (amount - 1), [1] * (amount - 1)
    while rest > 0:
        free = [i for i in range(amount - 1) if given[i] < bound]
        mass, budget = sum([loads[i] for i in free]), rest
        for i in free:
            more = min(bound - given[i], max(1, budget * loads[i] // mass), rest)
            given[i] = given[i] + more
            rest = rest - more
    return np.array([bound] + given)


def ragged_sizes(key, amount, total, reach, slope):
    if amount == 2:
        one = jax.random.randint(key, (), max(1, total - reach), min(reach, total - 1) + 1)
        return jnp.stack([one, total - one])
    sizes = jnp.asarray(profile(amount, total, reach, slope), jnp.int32)
    couples = (amount - 1) // 2
    giver, sink = sizes[1:1 + 2 * couples:2], sizes[2:2 + 2 * couples:2]
    margin = jnp.minimum(giver - 1, reach - sink)
    passed = jax.random.randint(jax.random.fold_in(key, 1), (couples,), 0, 1 << 20) % (margin + 1)
    sizes = sizes.at[1:1 + 2 * couples:2].set(giver - passed).at[2:2 + 2 * couples:2].set(sink + passed)
    return sizes[jax.random.permutation(jax.random.fold_in(key, 2), amount)]


def bell_draw(stream_key, extent, deviation, bound, shards=(), held_as=jnp.bfloat16):
    values = jax.random.normal(stream_key, extent, jnp.float32) * deviation
    if len(shards) > 0:
        values = block_levels(stream_key, extent, shards, -0.22, 0.18) * values
    return jnp.clip(values, min=-bound, max=bound).astype(held_as)


def setup_inputs(seed: int = 0) -> dict:
    key_of = jax.random.split(jax.random.key(seed), 5)
    queries = draw_queries(jax.random.fold_in(key_of[4], 71), 0)
    key_rows = draw_key_rows(jax.random.fold_in(key_of[4], 71), 0)
    value_rows = bell_draw(key_of[2], (BLOCKS, BLOCK_LEN, KV_HEADS * HEAD_DIM), 1.0, 6.0, ((0, 4), (1, 8)))
    tile_segment = jnp.searchsorted(jnp.cumsum(ragged_sizes(key_of[3], TILES // 4, TILES, 8, 0)), jnp.arange(TILES), side="right").astype(jnp.int32)
    return dict(queries=queries, key_rows=key_rows, value_rows=value_rows, tile_segment=tile_segment)


masked_score = -1.0e30


def visible(query_pos, query_seg, key_pos, key_seg):
    earlier = key_pos[None, :] <= query_pos[:, None]
    same_image = (key_seg[None, :] == query_seg[:, None]) & (query_seg[:, None] % 2 == 1)
    return earlier | same_image


def reference(queries, key_rows, value_rows, tile_segment):
    seq_total = queries.shape[0] * queries.shape[1]
    group_size = Q_HEADS // KV_HEADS
    query_flat = queries.reshape(seq_total, KV_HEADS, group_size, HEAD_DIM)
    key_flat = key_rows.reshape(seq_total, KV_HEADS, HEAD_DIM).astype(jnp.float32)
    value_flat = value_rows.reshape(seq_total, KV_HEADS, HEAD_DIM).astype(jnp.float32)
    positions = jnp.arange(seq_total, dtype=jnp.int32)
    segments = tile_segment[positions // TILE]
    block_rows = math.gcd(seq_total, 128)
    score_scale = HEAD_DIM ** -0.5

    def one_block(block_index):
        begin = (block_index * block_rows).astype(jnp.int32)
        query_block = lax.dynamic_slice_in_dim(query_flat, begin, block_rows, 0).astype(jnp.float32)
        query_pos = begin + jnp.arange(block_rows, dtype=jnp.int32)
        query_seg = lax.dynamic_slice_in_dim(segments, begin, block_rows, 0)
        allowed = visible(query_pos, query_seg, positions, segments)
        scores = jnp.einsum("qkgd,skd->kgqs", query_block, key_flat) * score_scale
        scores = jnp.where(allowed[None, None], scores, masked_score)
        new_max = jnp.max(scores, axis=3)
        weights = jnp.where(allowed[None, None], jnp.exp(scores - new_max[..., None]), 0.0)
        denominators = jnp.sum(weights, axis=3)
        rounded = lax.optimization_barrier(weights.astype(jnp.bfloat16))
        mixed = jnp.einsum("kgqs,skd->kgqd", rounded.astype(jnp.float32), value_flat) / denominators[..., None]
        return jnp.transpose(mixed, (2, 0, 1, 3)).reshape(block_rows, Q_HEADS * HEAD_DIM).astype(jnp.bfloat16)

    blocks_out = lax.map(one_block, jnp.arange(seq_total // block_rows, dtype=jnp.int32))
    return blocks_out.reshape(queries.shape)
```

```python
import functools
import math

import jax
import jax.numpy as jnp
from jax import lax
from jax.experimental import pallas as pl
from jax.experimental.pallas import tpu as pltpu
from jax.sharding import PartitionSpec as P

HEAD_DIM = 128
TILE = 128
MASKED = -1e30
MESH = pl.DeviceIdType.MESH


def kernel(
    dims, q_ref, k_ref, v_ref, seg_ref, out_ref,
    kv, qb, ob, m_ref, acc_ref,
    kv_recv, kv_send, chain_send, q_recv, q_send, o_recv, o_send,
):
    ulysses, blocks, hx, hb = dims
    peers = hx * hb
    gu_n, gb_n = ulysses // hx, blocks // hb
    planes = gu_n * gb_n
    rows = q_ref.shape[1]
    width = q_ref.shape[2] // peers
    group = width // HEAD_DIM
    block_len = rows * ulysses
    tile_rows = rows * hx
    scale = HEAD_DIM ** -0.5 * math.log2(math.e)

    u, b = lax.axis_index("ulysses"), lax.axis_index("blk")
    gu, gb = u // hx, b // hb
    g = gb * gu_n + gu
    me = (b % hb) * hx + u % hx

    def peer_id(p):
        return (gu * hx + p % hx, gb * hb + p // hx)

    def plane_id(other):
        return ((other % gu_n) * hx + u % hx, (other // gu_n) * hb + b % hb)

    barrier = pltpu.get_barrier_semaphore()
    for j in range(1, peers):
        pl.semaphore_signal(
            barrier, inc=1, device_id=peer_id((me + j) % peers), device_id_type=MESH
        )

    @pl.when(g > 0)
    def _():
        pl.semaphore_signal(barrier, inc=1, device_id=plane_id(g - 1), device_id_type=MESH)

    @pl.when(g < planes - 1)
    def _():
        pl.semaphore_signal(barrier, inc=1, device_id=plane_id(g + 1), device_id_type=MESH)

    ends = jnp.where(g > 0, 1, 0) + jnp.where(g < planes - 1, 1, 0)
    pl.semaphore_wait(barrier, peers - 1 + ends)

    def columns(p, wide):
        return pl.ds(pl.multiple_of(p * wide, wide), wide)

    def remote(src, dst, send, recv, device):
        return pltpu.make_async_remote_copy(
            src_ref=src, dst_ref=dst, send_sem=send, recv_sem=recv,
            device_id=device, device_id_type=MESH,
        )

    for j in range(1, peers):
        p = (me + j) % peers
        for part, source in enumerate((k_ref, v_ref)):
            remote(
                source.at[0, :, columns(p, HEAD_DIM)], kv.at[g, me, part],
                kv_send.at[j], kv_recv.at[g, me], peer_id(p),
            ).start()

    def pass_own(target, send):
        for part, source in enumerate((k_ref, v_ref)):
            remote(
                source.at[0, :, columns(me, HEAD_DIM)], kv.at[g, me, part],
                send, kv_recv.at[g, me], plane_id(target),
            ).start()

    def pass_on(slot, piece, target, send):
        remote(
            kv.at[slot, piece], kv.at[slot, piece],
            send, kv_recv.at[slot, piece], plane_id(target),
        ).start()

    @pl.when(g > 0)
    def _():
        pass_own(g - 1, chain_send.at[planes])

    @pl.when(g < planes - 1)
    def _():
        pass_own(g + 1, chain_send.at[g])

    for j in range(1, peers):
        p = (me + j) % peers
        remote(
            q_ref.at[0, :, columns(p, width)], qb.at[me],
            q_send.at[j], q_recv.at[me], peer_id(p),
        ).start()

    kv[g, me, 0] = k_ref[0, :, columns(me, HEAD_DIM)]
    kv[g, me, 1] = v_ref[0, :, columns(me, HEAD_DIM)]
    qb[me] = q_ref[0, :, columns(me, width)]
    m_ref[...] = jnp.full_like(m_ref, MASKED)
    acc_ref[...] = jnp.zeros_like(acc_ref)

    def arrived(ref, sem):
        pltpu.make_async_copy(ref, ref, sem).wait()

    for j in range(1, peers):
        p = (me + peers - j) % peers
        arrived(kv.at[g, p], kv_recv.at[g, p])

        @pl.when(g > 0)
        def _():
            pass_on(g, p, g - 1, chain_send.at[planes])

        @pl.when(g < planes - 1)
        def _():
            pass_on(g, p, g + 1, chain_send.at[g])

    for j in range(1, peers):
        p = (me + peers - j) % peers
        arrived(qb.at[p], q_recv.at[p])

    def first_position(plane, bb):
        return (plane // gu_n * hb + bb) * block_len + (plane % gu_n) * tile_rows

    delta = lax.broadcasted_iota(jnp.int32, (tile_rows, tile_rows), 1) - lax.broadcasted_iota(
        jnp.int32, (tile_rows, tile_rows), 0
    )

    def attend(slot, bb):
        query_first = first_position(g, bb)
        query_seg = seg_ref[query_first // TILE]
        keys = kv[slot, :, 0].reshape(hb * tile_rows, HEAD_DIM)
        values = kv[slot, :, 1].reshape(hb * tile_rows, HEAD_DIM)
        values = jnp.concatenate([values, jnp.ones_like(values)], axis=1)
        visible = []
        for kb in range(hb):
            key_first = first_position(slot, kb)
            key_seg = seg_ref[key_first // TILE]
            same = jnp.logical_and(key_seg == query_seg, query_seg % 2 == 1)
            limit = jnp.where(same, jnp.int32(2 ** 30), query_first - key_first)
            visible.append(delta <= limit)
        for head in range(group):
            query = qb[pl.ds(bb * hx, hx), :, head * HEAD_DIM:(head + 1) * HEAD_DIM]
            query = query.reshape(tile_rows, HEAD_DIM)
            scores = lax.dot_general(
                query, keys, (((1,), (1,)), ((), ())), preferred_element_type=jnp.float32
            )
            scores = jnp.concatenate(
                [
                    jnp.where(visible[kb], scores[:, kb * tile_rows:(kb + 1) * tile_rows], MASKED)
                    for kb in range(hb)
                ],
                axis=1,
            )
            old = m_ref[bb, head]
            new = jnp.maximum(old, jnp.max(scores, axis=1, keepdims=True))
            m_ref[bb, head] = new
            factor = jnp.exp2((old - new) * scale)
            weights = jnp.exp2((scores - new[:, :1]) * scale).astype(jnp.bfloat16)
            product = jnp.dot(weights, values, preferred_element_type=jnp.float32)
            acc_ref[bb, head] = (
                jnp.concatenate([factor, factor], axis=1) * acc_ref[bb, head] + product
            )

    def attend_all(slot):
        def one(bb, carry):
            attend(slot, bb)
            return carry

        lax.fori_loop(0, hb, one, 0)

    attend_all(g)

    near = jnp.minimum(g, planes - 1 - g)

    def step(t, carry):
        both = t <= 2 * near
        distance = jnp.where(both, (t + 1) // 2, t - near)
        below = jnp.where(both, t % 2 == 1, g > planes - 1 - g)
        slot = jnp.where(below, g - distance, g + distance)
        target = jnp.where(below, g + 1, g - 1)
        onward = jnp.logical_and(target >= 0, target < planes)
        for p in range(peers):
            arrived(kv.at[slot, p], kv_recv.at[slot, p])

            @pl.when(onward)
            def _():
                pass_on(slot, p, target, chain_send.at[slot])

        attend_all(slot)
        return carry

    lax.fori_loop(1, planes, step, 0)

    for bb in range(hb):
        for head in range(group):
            total = acc_ref[bb, head]
            ob[bb * hx:(bb + 1) * hx, :, head * HEAD_DIM:(head + 1) * HEAD_DIM] = (
                (total[:, :HEAD_DIM] / total[:, HEAD_DIM:])
                .astype(jnp.bfloat16)
                .reshape(hx, rows, HEAD_DIM)
            )
        for ux in range(hx):
            p = bb * hx + ux

            @pl.when(p != me)
            def _():
                remote(
                    ob.at[p], out_ref.at[0, :, columns(me, width)],
                    o_send.at[p], o_recv.at[me], peer_id(p),
                ).start()

    out_ref[0, :, columns(me, width)] = ob[me]
    for j in range(1, peers):
        p = (me + peers - j) % peers
        mine = out_ref.at[0, :, columns(p, width)]
        arrived(mine, o_recv.at[p])
    for j in range(1, peers):
        p = (me + j) % peers
        arrived(kv.at[g, p], kv_send.at[j])
        arrived(qb.at[p], q_send.at[j])
        arrived(ob.at[p], o_send.at[p])

    @pl.when(g > 0)
    def _():
        arrived(kv.at[g], chain_send.at[planes])

    @pl.when(g < planes - 1)
    def _():
        arrived(kv.at[g], chain_send.at[g])

    def drain(slot, carry):
        passed = jnp.logical_or(
            jnp.logical_and(slot < g, g < planes - 1), jnp.logical_and(slot > g, g > 0)
        )

        @pl.when(passed)
        def _():
            arrived(kv.at[slot], chain_send.at[slot])

        return carry

    lax.fori_loop(0, planes, drain, 0)


def local(queries, key_rows, value_rows, tile_segment):
    ulysses, blocks = lax.axis_size("ulysses"), lax.axis_size("blk")
    kv_heads = key_rows.shape[2] // HEAD_DIM
    rows = queries.shape[1]
    hb = math.gcd(blocks, max(1, kv_heads // 2))
    hx = kv_heads // hb
    planes = ulysses * blocks // kv_heads
    group = queries.shape[2] // HEAD_DIM // kv_heads
    tile_rows = hx * rows
    assert ulysses % hx == 0 and TILE % tile_rows == 0
    vmem = pl.BlockSpec(memory_space=pltpu.VMEM)
    dma = pltpu.SemaphoreType.DMA
    return pl.pallas_call(
        functools.partial(kernel, (ulysses, blocks, hx, hb)),
        out_shape=jax.ShapeDtypeStruct(queries.shape, jnp.bfloat16),
        in_specs=[vmem, vmem, vmem, pl.BlockSpec(memory_space=pltpu.SMEM)],
        out_specs=vmem,
        scratch_shapes=[
            pltpu.VMEM((planes, kv_heads, 2, rows, HEAD_DIM), jnp.bfloat16),
            pltpu.VMEM((kv_heads, rows, group * HEAD_DIM), jnp.bfloat16),
            pltpu.VMEM((kv_heads, rows, group * HEAD_DIM), jnp.bfloat16),
            pltpu.VMEM((hb, group, tile_rows, HEAD_DIM), jnp.float32),
            pltpu.VMEM((hb, group, tile_rows, 2 * HEAD_DIM), jnp.float32),
            dma((planes, kv_heads)),
            dma((kv_heads,)),
            dma((planes + 1,)),
            dma((kv_heads,)),
            dma((kv_heads,)),
            dma((kv_heads,)),
            dma((kv_heads,)),
        ],
        compiler_params=pltpu.CompilerParams(collective_id=0, has_side_effects=True),
    )(queries, key_rows, value_rows, tile_segment)


def solution(mesh):
    return jax.shard_map(
        local,
        mesh=mesh,
        in_specs=(
            P("blk", "ulysses", None),
            P("blk", "ulysses", None),
            P("blk", "ulysses", None),
            P(),
        ),
        out_specs=P("blk", "ulysses", None),
        check_vma=False,
    )
```

```python
import functools
import math

import jax
import jax.numpy as jnp
from jax import lax
from jax.experimental import pallas as pl
from jax.experimental.pallas import tpu as pltpu
from jax.sharding import PartitionSpec as P

HEAD_DIM = 128
TILE = 128
MASKED = -1e30
MESH = pl.DeviceIdType.MESH


def kernel(
    dims, q_ref, k_ref, v_ref, seg_ref, out_ref,
    kv, qb, qs, ob, m_ref, acc_ref,
    kv_recv, kv_send, chain_send, q_recv, q_send, o_recv, o_send,
):
    ulysses, blocks, hx, hb = dims
    peers = hx * hb
    gu_n, gb_n = ulysses // hx, blocks // hb
    planes = gu_n * gb_n
    rows = q_ref.shape[1]
    width = q_ref.shape[2] // peers
    group = width // HEAD_DIM
    block_len = rows * ulysses
    tile_rows = rows * hx
    scale = HEAD_DIM ** -0.5 * math.log2(math.e)

    u, b = lax.axis_index("ulysses"), lax.axis_index("blk")
    gu, gb = u // hx, b // hb
    g = gb * gu_n + gu
    me = (b % hb) * hx + u % hx

    def peer_id(p):
        return (gu * hx + p % hx, gb * hb + p // hx)

    def plane_id(other):
        return ((other % gu_n) * hx + u % hx, (other // gu_n) * hb + b % hb)

    barrier = pltpu.get_barrier_semaphore()
    for j in range(1, peers):
        pl.semaphore_signal(
            barrier, inc=1, device_id=peer_id((me + j) % peers), device_id_type=MESH
        )

    @pl.when(g > 0)
    def _():
        pl.semaphore_signal(barrier, inc=1, device_id=plane_id(g - 1), device_id_type=MESH)

    @pl.when(g < planes - 1)
    def _():
        pl.semaphore_signal(barrier, inc=1, device_id=plane_id(g + 1), device_id_type=MESH)

    ends = jnp.where(g > 0, 1, 0) + jnp.where(g < planes - 1, 1, 0)
    pl.semaphore_wait(barrier, peers - 1 + ends)

    def columns(p, wide):
        return pl.ds(pl.multiple_of(p * wide, wide), wide)

    def remote(src, dst, send, recv, device):
        return pltpu.make_async_remote_copy(
            src_ref=src, dst_ref=dst, send_sem=send, recv_sem=recv,
            device_id=device, device_id_type=MESH,
        )

    for j in range(1, peers):
        p = (me + j) % peers
        for part, source in enumerate((k_ref, v_ref)):
            remote(
                source.at[0, :, columns(p, HEAD_DIM)], kv.at[g, me, part],
                kv_send.at[j], kv_recv.at[g, me], peer_id(p),
            ).start()

    def pass_own(target, send):
        for part, source in enumerate((k_ref, v_ref)):
            remote(
                source.at[0, :, columns(me, HEAD_DIM)], kv.at[g, me, part],
                send, kv_recv.at[g, me], plane_id(target),
            ).start()

    def pass_on(slot, piece, target, send):
        remote(
            kv.at[slot, piece], kv.at[slot, piece],
            send, kv_recv.at[slot, piece], plane_id(target),
        ).start()

    @pl.when(g > 0)
    def _():
        pass_own(g - 1, chain_send.at[planes])

    @pl.when(g < planes - 1)
    def _():
        pass_own(g + 1, chain_send.at[g])

    for j in range(1, peers):
        p = (me + j) % peers
        remote(
            q_ref.at[0, :, columns(p, width)], qb.at[me],
            q_send.at[j], q_recv.at[me], peer_id(p),
        ).start()

    kv[g, me, 0] = k_ref[0, :, columns(me, HEAD_DIM)]
    kv[g, me, 1] = v_ref[0, :, columns(me, HEAD_DIM)]
    qb[me] = q_ref[0, :, columns(me, width)]
    m_ref[...] = jnp.full_like(m_ref, MASKED)
    acc_ref[...] = jnp.zeros_like(acc_ref)

    def arrived(ref, sem):
        pltpu.make_async_copy(ref, ref, sem).wait()

    for j in range(1, peers):
        p = (me + peers - j) % peers
        arrived(kv.at[g, p], kv_recv.at[g, p])

        @pl.when(g > 0)
        def _():
            pass_on(g, p, g - 1, chain_send.at[planes])

        @pl.when(g < planes - 1)
        def _():
            pass_on(g, p, g + 1, chain_send.at[g])

    for j in range(1, peers):
        p = (me + peers - j) % peers
        arrived(qb.at[p], q_recv.at[p])

    for p in range(peers):
        for head in range(group):
            low = head * tile_rows + (p % hx) * rows
            qs[p // hx, low:low + rows, :] = qb[p, :, head * HEAD_DIM:(head + 1) * HEAD_DIM]

    def first_position(plane, bb):
        return (plane // gu_n * hb + bb) * block_len + (plane % gu_n) * tile_rows

    delta = lax.broadcasted_iota(jnp.int32, (tile_rows, tile_rows), 1) - lax.broadcasted_iota(
        jnp.int32, (tile_rows, tile_rows), 0
    )

    def attend(slot, bb):
        query_first = first_position(g, bb)
        query_seg = seg_ref[query_first // TILE]
        keys = kv[slot, :, 0].reshape(hb * tile_rows, HEAD_DIM)
        values = kv[slot, :, 1].reshape(hb * tile_rows, HEAD_DIM)
        values = jnp.concatenate([values, jnp.ones_like(values)], axis=1)
        visible = []
        for kb in range(hb):
            key_first = first_position(slot, kb)
            key_seg = seg_ref[key_first // TILE]
            same = jnp.logical_and(key_seg == query_seg, query_seg % 2 == 1)
            limit = jnp.where(same, jnp.int32(2 ** 30), query_first - key_first)
            visible.append(delta <= limit)
        bound = jnp.where(jnp.concatenate(visible, axis=1), -MASKED, MASKED)
        scores = lax.dot_general(
            qs[bb], keys, (((1,), (1,)), ((), ())), preferred_element_type=jnp.float32
        )
        scores = jnp.minimum(scores, jnp.concatenate([bound] * group, axis=0))
        old = m_ref[bb]
        new = jnp.maximum(old, jnp.max(scores, axis=1, keepdims=True))
        m_ref[bb] = new
        factor = jnp.exp2((old - new) * scale)
        top = jnp.concatenate([new] * (scores.shape[1] // HEAD_DIM), axis=1)
        weights = jnp.exp2((scores - top) * scale).astype(jnp.bfloat16)
        product = jnp.dot(weights, values, preferred_element_type=jnp.float32)
        acc_ref[bb] = jnp.concatenate([factor, factor], axis=1) * acc_ref[bb] + product

    def attend_all(slot):
        def one(bb, carry):
            attend(slot, bb)
            return carry

        lax.fori_loop(0, hb, one, 0, unroll=True)

    attend_all(g)

    near = jnp.minimum(g, planes - 1 - g)

    def step(t, carry):
        both = t <= 2 * near
        distance = jnp.where(both, (t + 1) // 2, t - near)
        below = jnp.where(both, t % 2 == 1, g > planes - 1 - g)
        slot = jnp.where(below, g - distance, g + distance)
        target = jnp.where(below, g + 1, g - 1)
        onward = jnp.logical_and(target >= 0, target < planes)
        for p in range(peers):
            arrived(kv.at[slot, p], kv_recv.at[slot, p])

            @pl.when(onward)
            def _():
                pass_on(slot, p, target, chain_send.at[slot])

        attend_all(slot)
        return carry

    lax.fori_loop(1, planes, step, 0)

    for bb in range(hb):
        for head in range(group):
            total = acc_ref[bb, head * tile_rows:(head + 1) * tile_rows]
            ob[bb * hx:(bb + 1) * hx, :, head * HEAD_DIM:(head + 1) * HEAD_DIM] = (
                (total[:, :HEAD_DIM] / total[:, HEAD_DIM:])
                .astype(jnp.bfloat16)
                .reshape(hx, rows, HEAD_DIM)
            )
        for ux in range(hx):
            p = bb * hx + ux

            @pl.when(p != me)
            def _():
                remote(
                    ob.at[p], out_ref.at[0, :, columns(me, width)],
                    o_send.at[p], o_recv.at[me], peer_id(p),
                ).start()

    out_ref[0, :, columns(me, width)] = ob[me]
    for j in range(1, peers):
        p = (me + peers - j) % peers
        mine = out_ref.at[0, :, columns(p, width)]
        arrived(mine, o_recv.at[p])
    for j in range(1, peers):
        p = (me + j) % peers
        arrived(kv.at[g, p], kv_send.at[j])
        arrived(qb.at[p], q_send.at[j])
        arrived(ob.at[p], o_send.at[p])

    @pl.when(g > 0)
    def _():
        arrived(kv.at[g], chain_send.at[planes])

    @pl.when(g < planes - 1)
    def _():
        arrived(kv.at[g], chain_send.at[g])

    def drain(slot, carry):
        passed = jnp.logical_or(
            jnp.logical_and(slot < g, g < planes - 1), jnp.logical_and(slot > g, g > 0)
        )

        @pl.when(passed)
        def _():
            arrived(kv.at[slot], chain_send.at[slot])

        return carry

    lax.fori_loop(0, planes, drain, 0)


def local(queries, key_rows, value_rows, tile_segment):
    ulysses, blocks = lax.axis_size("ulysses"), lax.axis_size("blk")
    kv_heads = key_rows.shape[2] // HEAD_DIM
    rows = queries.shape[1]
    hb = math.gcd(blocks, max(1, kv_heads // 2))
    hx = kv_heads // hb
    planes = ulysses * blocks // kv_heads
    group = queries.shape[2] // HEAD_DIM // kv_heads
    tile_rows = hx * rows
    assert ulysses % hx == 0 and TILE % tile_rows == 0
    vmem = pl.BlockSpec(memory_space=pltpu.VMEM)
    dma = pltpu.SemaphoreType.DMA
    return pl.pallas_call(
        functools.partial(kernel, (ulysses, blocks, hx, hb)),
        out_shape=jax.ShapeDtypeStruct(queries.shape, jnp.bfloat16),
        in_specs=[vmem, vmem, vmem, pl.BlockSpec(memory_space=pltpu.SMEM)],
        out_specs=vmem,
        scratch_shapes=[
            pltpu.VMEM((planes, kv_heads, 2, rows, HEAD_DIM), jnp.bfloat16),
            pltpu.VMEM((kv_heads, rows, group * HEAD_DIM), jnp.bfloat16),
            pltpu.VMEM((hb, group * tile_rows, HEAD_DIM), jnp.bfloat16),
            pltpu.VMEM((kv_heads, rows, group * HEAD_DIM), jnp.bfloat16),
            pltpu.VMEM((hb, group * tile_rows, HEAD_DIM), jnp.float32),
            pltpu.VMEM((hb, group * tile_rows, 2 * HEAD_DIM), jnp.float32),
            dma((planes, kv_heads)),
            dma((kv_heads,)),
            dma((planes + 1,)),
            dma((kv_heads,)),
            dma((kv_heads,)),
            dma((kv_heads,)),
            dma((kv_heads,)),
        ],
        compiler_params=pltpu.CompilerParams(collective_id=0, has_side_effects=True),
    )(queries, key_rows, value_rows, tile_segment)


def solution(mesh):
    return jax.shard_map(
        local,
        mesh=mesh,
        in_specs=(
            P("blk", "ulysses", None),
            P("blk", "ulysses", None),
            P("blk", "ulysses", None),
            P(),
        ),
        out_specs=P("blk", "ulysses", None),
        check_vma=False,
    )
```

```python
import functools
import math

import jax
import jax.numpy as jnp
from jax import lax
from jax.experimental import pallas as pl
from jax.experimental.pallas import tpu as pltpu
from jax.sharding import PartitionSpec as P

HEAD_DIM = 128
TILE = 128
MASKED = -1e30
MESH = pl.DeviceIdType.MESH


def kernel(
    dims, q_hbm, k_hbm, v_hbm, seg_ref, out_ref,
    q_ref, k_ref, v_ref, kv, qb, qs, ob, m_ref, acc_ref,
    in_sems, kv_recv, kv_send, chain_send, q_recv, q_send, o_recv, o_send,
):
    ulysses, blocks, hx, hb = dims
    peers = hx * hb
    gu_n, gb_n = ulysses // hx, blocks // hb
    planes = gu_n * gb_n
    rows = q_ref.shape[1]
    width = q_ref.shape[2] // peers
    group = width // HEAD_DIM
    block_len = rows * ulysses
    tile_rows = rows * hx
    scale = HEAD_DIM ** -0.5 * math.log2(math.e)

    u, b = lax.axis_index("ulysses"), lax.axis_index("blk")
    gu, gb = u // hx, b // hb
    g = gb * gu_n + gu
    me = (b % hb) * hx + u % hx

    def peer_id(p):
        return (gu * hx + p % hx, gb * hb + p // hx)

    def plane_id(other):
        return ((other % gu_n) * hx + u % hx, (other // gu_n) * hb + b % hb)

    loads = [
        pltpu.make_async_copy(source, held, in_sems.at[i])
        for i, (source, held) in enumerate(((k_hbm, k_ref), (v_hbm, v_ref), (q_hbm, q_ref)))
    ]
    for load in loads:
        load.start()

    barrier = pltpu.get_barrier_semaphore()
    for j in range(1, peers):
        pl.semaphore_signal(
            barrier, inc=1, device_id=peer_id((me + j) % peers), device_id_type=MESH
        )

    @pl.when(g > 0)
    def _():
        pl.semaphore_signal(barrier, inc=1, device_id=plane_id(g - 1), device_id_type=MESH)

    @pl.when(g < planes - 1)
    def _():
        pl.semaphore_signal(barrier, inc=1, device_id=plane_id(g + 1), device_id_type=MESH)

    m_ref[...] = jnp.full_like(m_ref, MASKED)
    acc_ref[...] = jnp.zeros_like(acc_ref)
    loads[0].wait()
    loads[1].wait()

    ends = jnp.where(g > 0, 1, 0) + jnp.where(g < planes - 1, 1, 0)
    pl.semaphore_wait(barrier, peers - 1 + ends)

    def columns(p, wide):
        return pl.ds(pl.multiple_of(p * wide, wide), wide)

    def remote(src, dst, send, recv, device):
        return pltpu.make_async_remote_copy(
            src_ref=src, dst_ref=dst, send_sem=send, recv_sem=recv,
            device_id=device, device_id_type=MESH,
        )

    for j in range(1, peers):
        p = (me + j) % peers
        for part, source in enumerate((k_ref, v_ref)):
            remote(
                source.at[0, :, columns(p, HEAD_DIM)], kv.at[g, me, part],
                kv_send.at[j], kv_recv.at[g, me], peer_id(p),
            ).start()

    def pass_own(target, send):
        for part, source in enumerate((k_ref, v_ref)):
            remote(
                source.at[0, :, columns(me, HEAD_DIM)], kv.at[g, me, part],
                send, kv_recv.at[g, me], plane_id(target),
            ).start()

    def pass_on(slot, piece, target, send):
        remote(
            kv.at[slot, piece], kv.at[slot, piece],
            send, kv_recv.at[slot, piece], plane_id(target),
        ).start()

    @pl.when(g > 0)
    def _():
        pass_own(g - 1, chain_send.at[planes])

    @pl.when(g < planes - 1)
    def _():
        pass_own(g + 1, chain_send.at[g])

    loads[2].wait()
    for j in range(1, peers):
        p = (me + j) % peers
        remote(
            q_ref.at[0, :, columns(p, width)], qb.at[me],
            q_send.at[j], q_recv.at[me], peer_id(p),
        ).start()

    kv[g, me, 0] = k_ref[0, :, columns(me, HEAD_DIM)]
    kv[g, me, 1] = v_ref[0, :, columns(me, HEAD_DIM)]
    qb[me] = q_ref[0, :, columns(me, width)]

    def arrived(ref, sem):
        pltpu.make_async_copy(ref, ref, sem).wait()

    for j in range(1, peers):
        p = (me + peers - j) % peers
        arrived(kv.at[g, p], kv_recv.at[g, p])

        @pl.when(g > 0)
        def _():
            pass_on(g, p, g - 1, chain_send.at[planes])

        @pl.when(g < planes - 1)
        def _():
            pass_on(g, p, g + 1, chain_send.at[g])

    near = jnp.minimum(g, planes - 1 - g)
    inner = jnp.logical_and(g > 0, g < planes - 1)

    def place(t):
        both = t <= 2 * near
        distance = jnp.where(both, (t + 1) // 2, t - near)
        below = jnp.where(both, t % 2 == 1, g > planes - 1 - g)
        return jnp.where(below, g - distance, g + distance), jnp.where(below, g + 1, g - 1)

    def take(t, half, when):
        @pl.when(when)
        def _():
            slot, target = place(t)
            for p in range(half * peers // 2, (half + 1) * peers // 2):
                arrived(kv.at[slot, p], kv_recv.at[slot, p])

                @pl.when(inner)
                def _():
                    pass_on(slot, p, target, chain_send.at[slot])

    for half in range(2):
        take(jnp.int32(1), half, planes > 1)

    for j in range(1, peers):
        p = (me + peers - j) % peers
        arrived(qb.at[p], q_recv.at[p])

    for p in range(peers):
        for head in range(group):
            low = head * tile_rows + (p % hx) * rows
            qs[p // hx, low:low + rows, :] = qb[p, :, head * HEAD_DIM:(head + 1) * HEAD_DIM]

    def first_position(plane, bb):
        return (plane // gu_n * hb + bb) * block_len + (plane % gu_n) * tile_rows

    delta = lax.broadcasted_iota(jnp.int32, (tile_rows, tile_rows), 1) - lax.broadcasted_iota(
        jnp.int32, (tile_rows, tile_rows), 0
    )

    def attend(slot, bb, low, high):
        query_first = first_position(g, bb)
        query_seg = seg_ref[query_first // TILE]
        keys = kv[slot, low * hx:high * hx, 0].reshape(-1, HEAD_DIM)
        values = kv[slot, low * hx:high * hx, 1].reshape(-1, HEAD_DIM)
        values = jnp.concatenate([values, jnp.ones_like(values)], axis=1)
        visible = []
        for kb in range(low, high):
            key_first = first_position(slot, kb)
            key_seg = seg_ref[key_first // TILE]
            same = jnp.logical_and(key_seg == query_seg, query_seg % 2 == 1)
            limit = jnp.where(same, jnp.int32(2 ** 30), query_first - key_first)
            visible.append(delta <= limit)
        bound = jnp.where(jnp.concatenate(visible, axis=1), -MASKED, MASKED)
        scores = lax.dot_general(
            qs[bb], keys, (((1,), (1,)), ((), ())), preferred_element_type=jnp.float32
        )
        scores = jnp.minimum(scores, jnp.concatenate([bound] * group, axis=0))
        old = m_ref[bb]
        new = jnp.maximum(old, jnp.max(scores, axis=1, keepdims=True))
        m_ref[bb] = new
        factor = jnp.exp2((old - new) * scale)
        top = jnp.concatenate([new] * (scores.shape[1] // HEAD_DIM), axis=1)
        weights = jnp.exp2((scores - top) * scale).astype(jnp.bfloat16)
        product = jnp.dot(weights, values, preferred_element_type=jnp.float32)
        acc_ref[bb] = jnp.concatenate([factor, factor], axis=1) * acc_ref[bb] + product

    def step(t, carry):
        for half in range(2):
            take(t, half, jnp.logical_and(t > 1, jnp.logical_not(inner)))
        later = jnp.logical_and(t + 2 < planes, inner)
        take(t + 2, 0, later)
        slot = jnp.where(t == 0, g, place(t)[0])
        for bb in range(hb):
            attend(slot, bb, 0, hb)
        take(t + 2, 1, later)
        return carry

    lax.fori_loop(0, planes - 1, step, 0)

    last = planes - 1
    wait_last = jnp.logical_and(last > 1, jnp.logical_not(inner))
    slot = place(last)[0]
    take(last, 0, wait_last)
    for bb in range(hb):
        attend(slot, bb, 0, hb // 2)
    take(last, 1, wait_last)

    def finish(bb):
        for head in range(group):
            total = acc_ref[bb, head * tile_rows:(head + 1) * tile_rows]
            ob[bb * hx:(bb + 1) * hx, :, head * HEAD_DIM:(head + 1) * HEAD_DIM] = (
                (total[:, :HEAD_DIM] / total[:, HEAD_DIM:])
                .astype(jnp.bfloat16)
                .reshape(hx, rows, HEAD_DIM)
            )

    def give(bb):
        for ux in range(hx):
            p = bb * hx + ux

            @pl.when(p != me)
            def _():
                remote(
                    ob.at[p], out_ref.at[0, :, columns(me, width)],
                    o_send.at[p], o_recv.at[me], peer_id(p),
                ).start()

    spread = max(1, hb // 2)
    for first in range(spread):
        share = range(first, hb, spread)
        for bb in share:
            attend(slot, bb, hb // 2, hb)
        for bb in share:
            finish(bb)
        for bb in share:
            give(bb)

    out_ref[0, :, columns(me, width)] = ob[me]
    for j in range(1, peers):
        p = (me + peers - j) % peers
        mine = out_ref.at[0, :, columns(p, width)]
        arrived(mine, o_recv.at[p])
    for j in range(1, peers):
        p = (me + j) % peers
        arrived(kv.at[g, p], kv_send.at[j])
        arrived(qb.at[p], q_send.at[j])
        arrived(ob.at[p], o_send.at[p])

    @pl.when(g > 0)
    def _():
        arrived(kv.at[g], chain_send.at[planes])

    @pl.when(g < planes - 1)
    def _():
        arrived(kv.at[g], chain_send.at[g])

    def drain(slot, carry):
        passed = jnp.logical_or(
            jnp.logical_and(slot < g, g < planes - 1), jnp.logical_and(slot > g, g > 0)
        )

        @pl.when(passed)
        def _():
            arrived(kv.at[slot], chain_send.at[slot])

        return carry

    lax.fori_loop(0, planes, drain, 0)


def local(queries, key_rows, value_rows, tile_segment):
    ulysses, blocks = lax.axis_size("ulysses"), lax.axis_size("blk")
    kv_heads = key_rows.shape[2] // HEAD_DIM
    rows = queries.shape[1]
    hb = math.gcd(blocks, max(1, kv_heads // 2))
    hx = kv_heads // hb
    planes = ulysses * blocks // kv_heads
    group = queries.shape[2] // HEAD_DIM // kv_heads
    tile_rows = hx * rows
    assert ulysses % hx == 0 and planes > 1 and hb % 2 == 0 and TILE % tile_rows == 0
    vmem = pl.BlockSpec(memory_space=pltpu.VMEM)
    hbm = pl.BlockSpec(memory_space=pl.ANY)
    dma = pltpu.SemaphoreType.DMA
    return pl.pallas_call(
        functools.partial(kernel, (ulysses, blocks, hx, hb)),
        out_shape=pltpu.VMEM(queries.shape, jnp.bfloat16),
        in_specs=[hbm, hbm, hbm, pl.BlockSpec(memory_space=pltpu.SMEM)],
        out_specs=vmem,
        scratch_shapes=[
            pltpu.VMEM(queries.shape, jnp.bfloat16),
            pltpu.VMEM(key_rows.shape, jnp.bfloat16),
            pltpu.VMEM(value_rows.shape, jnp.bfloat16),
            pltpu.VMEM((planes, kv_heads, 2, rows, HEAD_DIM), jnp.bfloat16),
            pltpu.VMEM((kv_heads, rows, group * HEAD_DIM), jnp.bfloat16),
            pltpu.VMEM((hb, group * tile_rows, HEAD_DIM), jnp.bfloat16),
            pltpu.VMEM((kv_heads, rows, group * HEAD_DIM), jnp.bfloat16),
            pltpu.VMEM((hb, group * tile_rows, HEAD_DIM), jnp.float32),
            pltpu.VMEM((hb, group * tile_rows, 2 * HEAD_DIM), jnp.float32),
            dma((3,)),
            dma((planes, kv_heads)),
            dma((kv_heads,)),
            dma((planes + 1,)),
            dma((kv_heads,)),
            dma((kv_heads,)),
            dma((kv_heads,)),
            dma((kv_heads,)),
        ],
        compiler_params=pltpu.CompilerParams(collective_id=0, has_side_effects=True),
    )(queries, key_rows, value_rows, tile_segment)


def solution(mesh):
    return jax.shard_map(
        local,
        mesh=mesh,
        in_specs=(
            P("blk", "ulysses", None),
            P("blk", "ulysses", None),
            P("blk", "ulysses", None),
            P(),
        ),
        out_specs=P("blk", "ulysses", None),
        check_vma=False,
    )
```
